32 devices in a mesh: ctx: 8 (over z, core), grp: 4 (over y, x).
Axes of the slice: x: 2, y: 2, z: 4, core: 2. Of those that a mesh axis runs over, the one named last changes fastest.
Arguments:
- queries: bfloat16 [2048, 8192], P('ctx', 'grp'), may hold values from -27 to 27, as said below
- keys: bfloat16 [2048, 1024], P('ctx'), may hold values from -27 to 27
- values: bfloat16 [2048, 1024], P('ctx'), may hold values from -6 to 6
- out_weight: bfloat16 [8192, 8192], P('grp'), may hold values from -0.0625 to 0.0625
- span_order: int32 [16], replicated, may hold values from 0 to 15, each once
- document: int32 [2048], replicated, may hold values from 0 to 3, never falling along the last dimension, each value on 1 to 1024 neighbouring positions
Outputs:
- projected: bfloat16 [2048, 8192], P('ctx', 'grp')
The draws below stay inside these ranges and needn't reach their ends.
Inputs may be any that keep to these rules, and one draw needn't show every extreme that they name: `queries`: queries and keys are of order one, except a few rows that may be larger.
All inputs are finite; a program needn't handle non-finite values.
Results may differ from the reference program's by a relative error of at most 0.023.
Values may be sent and summed in bfloat16 or wider, within the bound.
A program may use at most 128 MiB of HBM per device.

```python
import math
import jax
import jax.numpy as jnp
import numpy as np
from jax import lax

MODEL_DIM = 8192
Q_HEADS = 64
KV_HEADS = 8
HEAD_DIM = 128
QUERY_GROUP = 8
SPAN = 128
SEQ = 2048
N_CTX = 8
N_GRP = 4


def drawn_fields(key):
    base_query = jnp.clip(jax.random.normal(jax.random.fold_in(key, 11), (SEQ, Q_HEADS * HEAD_DIM), jnp.float32), -5.0, 5.0)
    base_key = jnp.clip(jax.random.normal(jax.random.fold_in(key, 12), (SEQ, KV_HEADS * HEAD_DIM), jnp.float32), -5.0, 5.0)
    return (base_query, base_key)


def draw_queries(key, part):
    return drawn_fields(key)[0].astype(jnp.bfloat16)


def draw_keys(key, part):
    return drawn_fields(key)[1].astype(jnp.bfloat16)


def block_scale(rng, dims, shards, low, top_value):
    factor_of, own = 1.0, jax.random.fold_in(rng, 6)
    for axis_at, blocks in shards:
        heights = jnp.exp(jax.random.uniform(jax.random.fold_in(own, axis_at), (blocks,), jnp.float32, low / len(shards), top_value / len(shards)))
        factor_of = factor_of * jnp.repeat(heights, dims[axis_at] // blocks).reshape([-1 if axis == axis_at else 1 for axis in range(len(dims))])
    return factor_of


def split_up(count, total, limit, skew):
    loads = [(1 << 20) // math.isqrt(rank ** skew) + 1 for rank in range(2, count + 1)]
    rest, counts = total - limit - (count - 1), [1] * (count - 1)
    while rest > 0:
        movable = [i for i in range(count - 1) if counts[i] < limit]
        mass, budget = sum([loads[i] for i in movable]), rest
        for i in movable:
            more = min(limit - counts[i], max(1, budget * loads[i] // mass), rest)
            counts[i] = counts[i] + more
            rest = rest - more
    return np.array([limit] + counts)


def ragged_sizes(own_key, number_of, total, reach, lean):
    if number_of == 2:
        one = jax.random.randint(own_key, (), max(1, total - reach), min(reach, total - 1) + 1)
        return jnp.stack([one, total - one])
    sizes = jnp.asarray(split_up(number_of, total, reach, lean), jnp.int32)
    twos = (number_of - 1) // 2
    donor, sink = sizes[1:1 + 2 * twos:2], sizes[2:2 + 2 * twos:2]
    slack = jnp.minimum(donor - 1, reach - sink)
    passed = jax.random.randint(jax.random.fold_in(own_key, 1), (twos,), 0, 1 << 20) % (slack + 1)
    sizes = sizes.at[1:1 + 2 * twos:2].set(donor - passed).at[2:2 + 2 * twos:2].set(sink + passed)
    return sizes[jax.random.permutation(jax.random.fold_in(own_key, 2), number_of)]


def bell_draw(own_key, dims, deviation, limit, cuts=(), kind=jnp.bfloat16):
    entries = deviation * jax.random.normal(own_key, dims, jnp.float32)
    if cuts:
        entries = entries * block_scale(own_key, dims, cuts, -0.22, 0.18)
    return jnp.clip(entries, -limit, limit).astype(kind)


def setup_inputs(seed: int = 0) -> dict:
    seeds = jax.random.split(jax.random.key(seed), 7)
    queries = draw_queries(jax.random.fold_in(seeds[6], 71), 0)
    keys = draw_keys(jax.random.fold_in(seeds[6], 71), 0)
    values = bell_draw(seeds[2], (SEQ, KV_HEADS * HEAD_DIM), 1.0, 6.0, ((0, 8),))
    out_weight = bell_draw(seeds[3], (Q_HEADS * HEAD_DIM, MODEL_DIM), (Q_HEADS * HEAD_DIM) ** -0.5, 0.0625, ((0, 4),))
    span_order = jax.random.permutation(seeds[4], 2 * N_CTX).astype(jnp.int32)
    document = jnp.searchsorted(jnp.cumsum(ragged_sizes(seeds[5], 4, SEQ, SEQ // 2, 0)), jnp.arange(SEQ), side="right").astype(jnp.int32)
    return dict(queries=queries, keys=keys, values=values, out_weight=out_weight, span_order=span_order, document=document)


def row_positions(span_order):
    rows = jnp.arange(SEQ, dtype=jnp.int32)
    return (span_order[rows // SPAN] * SPAN + rows % SPAN).astype(jnp.int32)

def reference(queries, keys, values, out_weight, span_order, document):
    positions = row_positions(span_order)
    docs = document[positions]
    visible = (positions[None, :] <= positions[:, None]) & (docs[None, :] == docs[:, None])
    score_scale = 1.0 / math.sqrt(HEAD_DIM)

    def one_head(head):
        shared = head // QUERY_GROUP
        query_head = lax.dynamic_slice_in_dim(queries, head * HEAD_DIM, HEAD_DIM, 1)
        key_head = lax.dynamic_slice_in_dim(keys, shared * HEAD_DIM, HEAD_DIM, 1)
        value_head = lax.dynamic_slice_in_dim(values, shared * HEAD_DIM, HEAD_DIM, 1)
        scores = jnp.dot(query_head, key_head.T, preferred_element_type=jnp.float32) * score_scale
        scores = jnp.where(visible, scores, -jnp.inf)
        highest = lax.optimization_barrier(jnp.max(scores, axis=1, keepdims=True))
        probs = jnp.exp(scores - highest)
        total = lax.optimization_barrier(jnp.sum(probs, axis=1, keepdims=True))
        mixed = jnp.dot(probs.astype(jnp.bfloat16), value_head, preferred_element_type=jnp.float32)
        return (mixed / total).astype(jnp.bfloat16)
    attended = lax.map(one_head, jnp.arange(Q_HEADS, dtype=jnp.int32))
    block_heads = Q_HEADS // N_GRP

    def add_block(running, block):
        head_rows = lax.dynamic_slice_in_dim(attended, block * block_heads, block_heads, 0)
        weight_rows = lax.dynamic_slice_in_dim(out_weight, block * block_heads * HEAD_DIM, block_heads * HEAD_DIM, 0)
        weight_rows = weight_rows.reshape(block_heads, HEAD_DIM, MODEL_DIM)
        block_sum = jnp.einsum('hsd,hdm->sm', head_rows.astype(jnp.float32), weight_rows.astype(jnp.float32))
        rounded = lax.optimization_barrier(block_sum.astype(jnp.bfloat16))
        return (running + rounded.astype(jnp.float32), None)
    start = jnp.zeros((SEQ, MODEL_DIM), jnp.float32)
    projected, unused = lax.scan(add_block, start, jnp.arange(N_GRP, dtype=jnp.int32))
    return projected.astype(jnp.bfloat16)
```

```python
import functools
import math

import jax
import jax.numpy as jnp
from jax import lax
from jax.experimental import pallas as pl
from jax.experimental.pallas import tpu as pltpu
from jax.sharding import PartitionSpec as P

HEAD_DIM = 128
QUERY_GROUP = 8
CORES = 2
MESH = pl.DeviceIdType.MESH
HIDDEN = -1e30


def gather_kernel(n_ctx, first_of, k_hbm, v_hbm, k_out, v_out, local_sem, send_sem, recv_sem):
    nz = n_ctx // CORES
    me = lax.axis_index("ctx")
    group = lax.axis_index("grp")
    z, core = me // CORES, me % CORES
    partner = z * CORES + 1 - core
    width = k_out.shape[2]
    start = pl.multiple_of(first_of(group) * HEAD_DIM, HEAD_DIM)
    outs = (k_out, v_out)
    loads = [
        pltpu.make_async_copy(src.at[:, pl.ds(start, width)], dst.at[me], local_sem.at[i])
        for i, (src, dst) in enumerate(((k_hbm, k_out), (v_hbm, v_out)))
    ]
    for load in loads:
        load.start()
    barrier = pltpu.get_barrier_semaphore()
    pl.semaphore_signal(barrier, inc=1, device_id=(partner, group), device_id_type=MESH)

    @pl.when(z > 0)
    def _():
        pl.semaphore_signal(barrier, inc=1, device_id=(me - CORES, group), device_id_type=MESH)

    @pl.when(z < nz - 1)
    def _():
        pl.semaphore_signal(barrier, inc=1, device_id=(me + CORES, group), device_id_type=MESH)

    pl.semaphore_wait(barrier, 1 + jnp.minimum(z, 1) + jnp.minimum(nz - 1 - z, 1))

    def piece(way, part, chip, target):
        block = chip * CORES + core
        return pltpu.make_async_remote_copy(
            src_ref=outs[part].at[block],
            dst_ref=outs[part].at[block],
            send_sem=send_sem.at[way, part, chip],
            recv_sem=recv_sem.at[part, block],
            device_id=(target, group),
            device_id_type=MESH,
        )

    for part in range(2):
        loads[part].wait()

        @pl.when(z < nz - 1)
        def _():
            piece(0, part, z, me + CORES).start()

        @pl.when(z > 0)
        def _():
            piece(1, part, z, me - CORES).start()

        piece(2, part, z, partner).start()

    def arrived(part, chip, from_core):
        block = chip * CORES + from_core
        pltpu.make_async_copy(
            outs[part].at[block], outs[part].at[block], recv_sem.at[part, block]
        ).wait()

    for k in range(nz - 1):
        for part in range(2):

            @pl.when(z - 1 - k >= 0)
            def _():
                arrived(part, z - 1 - k, core)

                @pl.when(z < nz - 1)
                def _():
                    piece(0, part, z - 1 - k, me + CORES).start()

                piece(2, part, z - 1 - k, partner).start()

            @pl.when(z + 1 + k < nz)
            def _():
                arrived(part, z + 1 + k, core)

                @pl.when(z > 0)
                def _():
                    piece(1, part, z + 1 + k, me - CORES).start()

                piece(2, part, z + 1 + k, partner).start()

    for part in range(2):
        for chip in range(nz):
            arrived(part, chip, 1 - core)
            piece(2, part, chip, partner).wait_send()

            @pl.when((z < nz - 1) & (chip <= z))
            def _():
                piece(0, part, chip, me + CORES).wait_send()

            @pl.when((z > 0) & (chip >= z))
            def _():
                piece(1, part, chip, me - CORES).wait_send()


def gather_kv(keys, values, n_ctx, kv_heads, first_of):
    rows = keys.shape[0]
    shape = jax.ShapeDtypeStruct((n_ctx, rows, kv_heads * HEAD_DIM), keys.dtype)
    return pl.pallas_call(
        functools.partial(gather_kernel, n_ctx, first_of),
        out_shape=(shape, shape),
        in_specs=[pl.BlockSpec(memory_space=pl.ANY)] * 2,
        out_specs=(pl.BlockSpec(memory_space=pltpu.VMEM),) * 2,
        scratch_shapes=[
            pltpu.SemaphoreType.DMA((2,)),
            pltpu.SemaphoreType.DMA((3, 2, n_ctx // CORES)),
            pltpu.SemaphoreType.DMA((2, n_ctx)),
        ],
        compiler_params=pltpu.CompilerParams(collective_id=0, has_side_effects=True),
        name="gather_kv",
    )(keys, values)


def attend_kernel(
    kv_heads, order_ref, doc_ref, doc_rows, q_ref, k_hbm, v_hbm, out_ref,
    k_pos, v_ext, bias_ref, max_ref, acc_ref, sems,
):
    slots, span = k_hbm.shape[0], k_hbm.shape[1]
    heads = q_ref.shape[1] // HEAD_DIM
    group = heads // kv_heads
    me = lax.axis_index("ctx")
    copies = []
    for slot in range(slots):
        at = order_ref[slot] + 1
        copies.append(pltpu.make_async_copy(k_hbm.at[slot], k_pos.at[at], sems.at[0, slot]))
        for h in range(kv_heads):
            copies.append(
                pltpu.make_async_copy(
                    v_hbm.at[slot, :, pl.ds(h * HEAD_DIM, HEAD_DIM)],
                    v_ext.at[h, at, :, pl.ds(0, HEAD_DIM)],
                    sems.at[1 + h, slot],
                )
            )
    for copy in copies:
        copy.start()
    k_pos[0] = jnp.zeros(k_pos.shape[1:], k_pos.dtype)
    for h in range(kv_heads):
        v_ext[h, :, :, HEAD_DIM:] = jnp.ones((slots + 1, span, HEAD_DIM), v_ext.dtype)
        v_ext[h, 0, :, :HEAD_DIM] = jnp.zeros((span, HEAD_DIM), v_ext.dtype)
    for copy in copies:
        copy.wait()

    factor = math.log2(math.e) / math.sqrt(HEAD_DIM)
    row_at = lax.broadcasted_iota(jnp.int32, (span, span), 0)
    col_at = lax.broadcasted_iota(jnp.int32, (span, span), 1)

    def one_span(r, carry):
        mine = order_ref[me * 2 + r]
        rows = pl.ds(pl.multiple_of(r * span, span), span)
        first_doc = doc_ref[mine * span]
        low = jnp.int32(0)
        for t in range(slots):
            low = low + (doc_ref[t * span + span - 1] < first_doc).astype(jnp.int32)
        blocks = (mine - low) // 2 + 1
        row_doc = jnp.transpose(jnp.broadcast_to(doc_rows[mine], (span, span)))

        def block_scores(b):
            top = mine - 2 * b
            for half in range(2):
                t = top - 1 + half
                key_doc = doc_rows[jnp.maximum(t, 0)]
                key_pos = t * span + col_at
                seen = (key_doc == row_doc) & (key_pos <= mine * span + row_at) & (key_pos >= 0)
                bias_ref[:, half * span : (half + 1) * span] = jnp.where(seen, 0.0, HIDDEN)
            bias = bias_ref[...]
            pair = k_pos[pl.ds(top, 2)].reshape(2 * span, kv_heads * HEAD_DIM)
            for h in range(kv_heads):
                q = jnp.concatenate(
                    [
                        q_ref[rows, (h * group + i) * HEAD_DIM : (h * group + i + 1) * HEAD_DIM]
                        for i in range(group)
                    ],
                    axis=0,
                )
                key = pair[:, h * HEAD_DIM : (h + 1) * HEAD_DIM]
                scores = lax.dot_general(
                    q, key, (((1,), (1,)), ((), ())), preferred_element_type=jnp.float32
                )
                value = v_ext[h, pl.ds(top, 2)].reshape(2 * span, 2 * HEAD_DIM)
                yield h, scores.reshape(group, span, 2 * span) + bias[None], value

        def mix(probs, value):
            low_probs = probs.astype(jnp.bfloat16).reshape(group * span, 2 * span)
            return jnp.dot(low_probs, value, preferred_element_type=jnp.float32)

        for h, scores, value in block_scores(0):
            top = jnp.max(scores, axis=-1, keepdims=True)
            max_ref[h] = jnp.broadcast_to(top, (group, span, HEAD_DIM))
            acc_ref[h] = mix(jnp.exp2((scores - top) * factor), value)

        def more(b, carry):
            for h, scores, value in block_scores(b):
                old = max_ref[h][:, :, :1]
                top = jnp.maximum(old, jnp.max(scores, axis=-1, keepdims=True))
                max_ref[h] = jnp.broadcast_to(top, (group, span, HEAD_DIM))
                rescale = jnp.exp2((old - top) * factor).reshape(group * span, 1)
                acc_ref[h] = acc_ref[h] * rescale + mix(jnp.exp2((scores - top) * factor), value)
            return carry

        lax.fori_loop(1, blocks, more, 0)
        for h in range(kv_heads):
            mixed = acc_ref[h]
            done = (mixed[:, :HEAD_DIM] / mixed[:, HEAD_DIM:]).astype(out_ref.dtype)
            for i in range(group):
                at = (h * group + i) * HEAD_DIM
                out_ref[rows, at : at + HEAD_DIM] = done[i * span : (i + 1) * span]
        return carry

    lax.fori_loop(0, 2, one_span, 0)


def attend(queries, key_all, value_all, span_order, document, kv_heads):
    slots = span_order.shape[0]
    span = document.shape[0] // slots
    group = queries.shape[1] // HEAD_DIM // kv_heads
    width = kv_heads * HEAD_DIM
    key_all = key_all.reshape(slots, span, width)
    value_all = value_all.reshape(slots, span, width)
    smem = pl.BlockSpec(memory_space=pltpu.SMEM)
    vmem = pl.BlockSpec(memory_space=pltpu.VMEM)
    hbm = pl.BlockSpec(memory_space=pl.ANY)
    return pl.pallas_call(
        functools.partial(attend_kernel, kv_heads),
        out_shape=jax.ShapeDtypeStruct(queries.shape, queries.dtype),
        in_specs=[smem, smem, vmem, vmem, hbm, hbm],
        out_specs=vmem,
        scratch_shapes=[
            pltpu.VMEM((slots + 1, span, width), jnp.bfloat16),
            pltpu.VMEM((kv_heads, slots + 1, span, 2 * HEAD_DIM), jnp.bfloat16),
            pltpu.VMEM((span, 2 * span), jnp.float32),
            pltpu.VMEM((kv_heads, group, span, HEAD_DIM), jnp.float32),
            pltpu.VMEM((kv_heads, group * span, 2 * HEAD_DIM), jnp.float32),
            pltpu.SemaphoreType.DMA((1 + kv_heads, slots)),
        ],
        name="attend",
    )(span_order, document, document.reshape(slots, 1, span), queries, key_all, value_all)


def project_kernel(
    att_ref, w_hbm, out_ref, w_buf, send_one, got_one, send_two, got_two, own_ref,
    w_sem, sent_one, recv_one, sent_two, recv_two,
):
    me = lax.axis_index("ctx")
    group = lax.axis_index("grp")
    side = group + 1 - 2 * (group % 2)
    other = (group + 2) % 4
    far = 3 - group
    steps, _, width = w_buf.shape
    block_width = out_ref.shape[1]

    def path_sub(i):
        path = i % 2
        return path, 2 * path + (i // 2) % 2

    def block_of(i):
        path = i % 2
        first = far if i < 4 else (other if path else side)
        return first if i < 8 else ((side if path else other) if i < 12 else group)

    def fetch(i, block, sub):
        start = pl.multiple_of(block * block_width + sub * width, width)
        return pltpu.make_async_copy(w_hbm.at[:, pl.ds(start, width)], w_buf.at[i], w_sem.at[i])

    for i in range(steps):
        fetch(i, block_of(i), path_sub(i)[1]).start()

    barrier = pltpu.get_barrier_semaphore()
    for target in (side, other):
        pl.semaphore_signal(barrier, inc=1, device_id=(me, target), device_id_type=MESH)
    pl.semaphore_wait(barrier, 2)

    def product(i):
        fetch(i, group, 0).wait()
        return jnp.dot(att_ref[...], w_buf[i], preferred_element_type=jnp.float32)

    def stage_one(i):
        path = i % 2
        return pltpu.make_async_remote_copy(
            src_ref=send_one.at[i],
            dst_ref=got_one.at[i],
            send_sem=sent_one.at[i],
            recv_sem=recv_one.at[i],
            device_id=(me, (1 - path) * side + path * other),
            device_id_type=MESH,
        )

    def stage_two(j):
        path = j % 2
        return pltpu.make_async_remote_copy(
            src_ref=send_two.at[j],
            dst_ref=got_two.at[j],
            send_sem=sent_two.at[j],
            recv_sem=recv_two.at[j],
            device_id=(me, (1 - path) * other + path * side),
            device_id_type=MESH,
        )

    def first(i, carry):
        send_one[i] = product(i).astype(send_one.dtype)
        stage_one(i).start()
        return carry

    lax.fori_loop(0, 8, first, 0)

    def second(j, carry):
        part = product(8 + j)
        stage_one(j).wait_recv()
        send_two[j] = (part + got_one[j].astype(jnp.float32)).astype(send_two.dtype)
        stage_two(j).start()
        return carry

    lax.fori_loop(0, 4, second, 0)

    def third(j, carry):
        own_ref[j] = product(12 + j)
        return carry

    lax.fori_loop(0, 4, third, 0)

    for j in range(4):
        stage_one(4 + j).wait_recv()
        own_ref[j] = own_ref[j] + got_one[4 + j].astype(jnp.float32)
    for j in range(4):
        stage_two(j).wait_recv()
        at = path_sub(j)[1] * width
        out_ref[:, at : at + width] = (own_ref[j] + got_two[j].astype(jnp.float32)).astype(
            out_ref.dtype
        )
    for i in range(8):
        stage_one(i).wait_send()
    for j in range(4):
        stage_two(j).wait_send()


def project(attended, out_weight):
    rows, depth = attended.shape
    features = out_weight.shape[1]
    width = features // 16
    bf16, f32 = jnp.bfloat16, jnp.float32
    return pl.pallas_call(
        project_kernel,
        out_shape=jax.ShapeDtypeStruct((rows, features // 4), bf16),
        in_specs=[pl.BlockSpec(memory_space=pltpu.VMEM), pl.BlockSpec(memory_space=pl.ANY)],
        out_specs=pl.BlockSpec(memory_space=pltpu.VMEM),
        scratch_shapes=[
            pltpu.VMEM((16, depth, width), bf16),
            pltpu.VMEM((8, rows, width), bf16),
            pltpu.VMEM((8, rows, width), bf16),
            pltpu.VMEM((4, rows, width), bf16),
            pltpu.VMEM((4, rows, width), bf16),
            pltpu.VMEM((4, rows, width), f32),
            pltpu.SemaphoreType.DMA((16,)),
            pltpu.SemaphoreType.DMA((8,)),
            pltpu.SemaphoreType.DMA((8,)),
            pltpu.SemaphoreType.DMA((4,)),
            pltpu.SemaphoreType.DMA((4,)),
        ],
        compiler_params=pltpu.CompilerParams(
            collective_id=1, has_side_effects=True, vmem_limit_bytes=60 * 1024 * 1024
        ),
        name="project",
    )(attended, out_weight)


def shards(n_ctx, n_grp, queries, keys, values, out_weight, span_order, document):
    local_heads = queries.shape[1] // HEAD_DIM
    kv_heads = max(1, local_heads // QUERY_GROUP)
    key_all, value_all = gather_kv(
        keys, values, n_ctx, kv_heads, lambda group: group * local_heads // QUERY_GROUP
    )
    attended = attend(queries, key_all, value_all, span_order, document, kv_heads)
    if n_grp == 4:
        return project(attended, out_weight)
    partial_value = jnp.dot(attended, out_weight, preferred_element_type=jnp.float32)
    return lax.psum_scatter(
        partial_value.astype(jnp.bfloat16), "grp", scatter_dimension=1, tiled=True
    )


def solution(mesh):
    in_specs = (P("ctx", "grp"), P("ctx", None), P("ctx", None), P("grp", None), P(), P())
    body = functools.partial(shards, mesh.shape["ctx"], mesh.shape["grp"])
    return jax.shard_map(
        body, mesh=mesh, in_specs=in_specs, out_specs=P("ctx", "grp"), check_vma=False
    )
```

```python
import functools
import math

import jax
import jax.numpy as jnp
from jax import lax
from jax.experimental import pallas as pl
from jax.experimental.pallas import tpu as pltpu
from jax.sharding import PartitionSpec as P

HEAD_DIM = 128
QUERY_GROUP = 8
CORES = 2
MESH = pl.DeviceIdType.MESH
HIDDEN = -1e30
UNROLL = 4


def gather_attend_kernel(
    n_ctx, kv_heads, first_of, order_ref, doc_rows, q_ref, k_hbm, v_hbm, out_ref,
    k_all, v_all, row_doc_ref, bias_ref, max_ref, acc_ref, local_sem, send_sem, recv_sem,
):
    nz = n_ctx // CORES
    me = lax.axis_index("ctx")
    group = lax.axis_index("grp")
    z, core = me // CORES, me % CORES
    partner = z * CORES + 1 - core
    tok_rows, width = k_all.shape[1], k_all.shape[2]
    span = tok_rows // 2
    heads = q_ref.shape[1] // HEAD_DIM
    shared = heads // kv_heads
    start = pl.multiple_of(first_of(group) * HEAD_DIM, HEAD_DIM)
    alls = (k_all, v_all)
    loads = [
        pltpu.make_async_copy(src.at[:, pl.ds(start, width)], dst.at[me], local_sem.at[i])
        for i, (src, dst) in enumerate(((k_hbm, k_all), (v_hbm, v_all)))
    ]
    for load in loads:
        load.start()
    barrier = pltpu.get_barrier_semaphore()
    pl.semaphore_signal(barrier, inc=1, device_id=(partner, group), device_id_type=MESH)

    @pl.when(z > 0)
    def _():
        pl.semaphore_signal(barrier, inc=1, device_id=(me - CORES, group), device_id_type=MESH)

    @pl.when(z < nz - 1)
    def _():
        pl.semaphore_signal(barrier, inc=1, device_id=(me + CORES, group), device_id_type=MESH)

    pl.semaphore_wait(barrier, 1 + jnp.minimum(z, 1) + jnp.minimum(nz - 1 - z, 1))

    def piece(way, part, chip, target):
        block = chip * CORES + core
        return pltpu.make_async_remote_copy(
            src_ref=alls[part].at[block],
            dst_ref=alls[part].at[block],
            send_sem=send_sem.at[way, part, chip],
            recv_sem=recv_sem.at[part, block],
            device_id=(target, group),
            device_id_type=MESH,
        )

    for part in range(2):
        loads[part].wait()

        @pl.when(z < nz - 1)
        def _():
            piece(0, part, z, me + CORES).start()

        @pl.when(z > 0)
        def _():
            piece(1, part, z, me - CORES).start()

        piece(2, part, z, partner).start()

    def arrived(part, chip, from_core):
        block = chip * CORES + from_core
        pltpu.make_async_copy(
            alls[part].at[block], alls[part].at[block], recv_sem.at[part, block]
        ).wait()

    max_ref[...] = jnp.full(max_ref.shape, HIDDEN, jnp.float32)
    acc_ref[...] = jnp.zeros(acc_ref.shape, jnp.float32)
    for r in range(2):
        row_doc_ref[r] = jnp.transpose(
            jnp.broadcast_to(doc_rows[order_ref[me * 2 + r]], (span, span))
        )

    factor = math.log2(math.e) / math.sqrt(HEAD_DIM)
    keys_per_step = CORES * tok_rows
    parts_of_keys = keys_per_step // HEAD_DIM
    row_at = lax.broadcasted_iota(jnp.int32, (span, span), 0)
    col_at = lax.broadcasted_iota(jnp.int32, (span, span), 1)
    near = jnp.minimum(z, nz - 1 - z)
    long_way = jnp.where(z < nz - 1 - z, 1, -1)

    def step(n, carry):
        for part in range(2):

            @pl.when((n > 0) & (z - n >= 0))
            def _():
                arrived(part, z - n, core)

                @pl.when(z < nz - 1)
                def _():
                    piece(0, part, z - n, me + CORES).start()

                piece(2, part, z - n, partner).start()

            @pl.when((n > 0) & (z + n < nz))
            def _():
                arrived(part, z + n, core)

                @pl.when(z > 0)
                def _():
                    piece(1, part, z + n, me - CORES).start()

                piece(2, part, z + n, partner).start()

        away = (n + 1) // 2
        paired = z + away * (1 - 2 * (n % 2))
        chip = jnp.where(n <= 2 * near, paired, z + long_way * (n - near))

        for slot in range(2 * CORES):
            key_span = order_ref[chip * (2 * CORES) + slot]
            key_doc = doc_rows[key_span]
            for r in range(2):
                mine = order_ref[me * 2 + r]
                seen = (key_doc == row_doc_ref[r]) & (
                    key_span * span + col_at <= mine * span + row_at
                )
                bias_ref[r * span : (r + 1) * span, slot * span : (slot + 1) * span] = jnp.where(
                    seen, 0.0, HIDDEN
                )

        for part in range(2):
            arrived(part, chip, 1 - core)

        for h in range(kv_heads):
            cols = slice(h * HEAD_DIM, (h + 1) * HEAD_DIM)

            def some_heads(at, carry):
                key = k_all[pl.ds(chip * CORES, CORES), :, cols].reshape(keys_per_step, HEAD_DIM)
                value = v_all[pl.ds(chip * CORES, CORES), :, cols].reshape(
                    keys_per_step, HEAD_DIM
                )
                value = jnp.concatenate([value, jnp.ones_like(value)], axis=1)
                picked = [h * shared + at * UNROLL + u for u in range(UNROLL)]
                scores = [
                    lax.dot_general(
                        q_ref[:, pl.ds(pl.multiple_of(head * HEAD_DIM, HEAD_DIM), HEAD_DIM)],
                        key,
                        (((1,), (1,)), ((), ())),
                        preferred_element_type=jnp.float32,
                    )
                    + bias_ref[...]
                    for head in picked
                ]
                olds = [max_ref[head] for head in picked]
                sums = [acc_ref[head] for head in picked]
                results = []
                for score, old, total in zip(scores, olds, sums):
                    top = jnp.maximum(old, jnp.max(score, axis=1, keepdims=True))
                    rescale = jnp.exp2((old - top) * factor)
                    probs = jnp.concatenate(
                        [
                            jnp.exp2(
                                (score[:, c * HEAD_DIM : (c + 1) * HEAD_DIM] - top) * factor
                            ).astype(jnp.bfloat16)
                            for c in range(parts_of_keys)
                        ],
                        axis=1,
                    )
                    mixed = jnp.dot(probs, value, preferred_element_type=jnp.float32)
                    both = jnp.concatenate([rescale, rescale], axis=1)
                    results.append((top, total * both + mixed))
                for head, (top, total) in zip(picked, results):
                    max_ref[head] = top
                    acc_ref[head] = total
                return carry

            lax.fori_loop(0, shared // UNROLL, some_heads, 0)
        return carry

    lax.fori_loop(0, nz, step, 0)

    for head in range(heads):
        total = acc_ref[head]
        out_ref[:, head * HEAD_DIM : (head + 1) * HEAD_DIM] = (
            total[:, :HEAD_DIM] / total[:, HEAD_DIM:]
        ).astype(out_ref.dtype)

    for part in range(2):
        for chip in range(nz):
            piece(2, part, chip, partner).wait_send()

            @pl.when((z < nz - 1) & (chip <= z))
            def _():
                piece(0, part, chip, me + CORES).wait_send()

            @pl.when((z > 0) & (chip >= z))
            def _():
                piece(1, part, chip, me - CORES).wait_send()


def gather_attend(queries, keys, values, span_order, document, n_ctx, kv_heads, first_of):
    slots = span_order.shape[0]
    span = document.shape[0] // slots
    rows = queries.shape[0]
    heads = queries.shape[1] // HEAD_DIM
    smem = pl.BlockSpec(memory_space=pltpu.SMEM)
    vmem = pl.BlockSpec(memory_space=pltpu.VMEM)
    hbm = pl.BlockSpec(memory_space=pl.ANY)
    f32, bf16 = jnp.float32, jnp.bfloat16
    return pl.pallas_call(
        functools.partial(gather_attend_kernel, n_ctx, kv_heads, first_of),
        out_shape=jax.ShapeDtypeStruct(queries.shape, queries.dtype),
        in_specs=[smem, vmem, vmem, hbm, hbm],
        out_specs=vmem,
        scratch_shapes=[
            pltpu.VMEM((n_ctx, rows, kv_heads * HEAD_DIM), bf16),
            pltpu.VMEM((n_ctx, rows, kv_heads * HEAD_DIM), bf16),
            pltpu.VMEM((2, span, span), jnp.int32),
            pltpu.VMEM((rows, CORES * rows), f32),
            pltpu.VMEM((heads, rows, HEAD_DIM), f32),
            pltpu.VMEM((heads, rows, 2 * HEAD_DIM), f32),
            pltpu.SemaphoreType.DMA((2,)),
            pltpu.SemaphoreType.DMA((3, 2, n_ctx // CORES)),
            pltpu.SemaphoreType.DMA((2, n_ctx)),
        ],
        compiler_params=pltpu.CompilerParams(collective_id=0, has_side_effects=True),
        name="gather_attend",
    )(span_order, document.reshape(slots, 1, span), queries, keys, values)


def project_kernel(
    att_ref, w_hbm, out_ref, w_buf, send_one, got_one, send_two, got_two, own_ref,
    w_sem, sent_one, recv_one, sent_two, recv_two,
):
    me = lax.axis_index("ctx")
    group = lax.axis_index("grp")
    side = group + 1 - 2 * (group % 2)
    other = (group + 2) % 4
    far = 3 - group
    steps, _, width = w_buf.shape
    block_width = out_ref.shape[1]

    def path_sub(i):
        path = i % 2
        return path, 2 * path + (i // 2) % 2

    def block_of(i):
        path = i % 2
        first = far if i < 4 else (other if path else side)
        return first if i < 8 else ((side if path else other) if i < 12 else group)

    def fetch(i, block, sub):
        start = pl.multiple_of(block * block_width + sub * width, width)
        return pltpu.make_async_copy(w_hbm.at[:, pl.ds(start, width)], w_buf.at[i], w_sem.at[i])

    for i in range(steps):
        fetch(i, block_of(i), path_sub(i)[1]).start()

    barrier = pltpu.get_barrier_semaphore()
    for target in (side, other):
        pl.semaphore_signal(barrier, inc=1, device_id=(me, target), device_id_type=MESH)
    pl.semaphore_wait(barrier, 2)

    def product(i):
        fetch(i, group, 0).wait()
        return jnp.dot(att_ref[...], w_buf[i], preferred_element_type=jnp.float32)

    def stage_one(i):
        path = i % 2
        return pltpu.make_async_remote_copy(
            src_ref=send_one.at[i],
            dst_ref=got_one.at[i],
            send_sem=sent_one.at[i],
            recv_sem=recv_one.at[i],
            device_id=(me, (1 - path) * side + path * other),
            device_id_type=MESH,
        )

    def stage_two(j):
        path = j % 2
        return pltpu.make_async_remote_copy(
            src_ref=send_two.at[j],
            dst_ref=got_two.at[j],
            send_sem=sent_two.at[j],
            recv_sem=recv_two.at[j],
            device_id=(me, (1 - path) * other + path * side),
            device_id_type=MESH,
        )

    def first(i, carry):
        send_one[i] = product(i).astype(send_one.dtype)
        stage_one(i).start()
        return carry

    lax.fori_loop(0, 8, first, 0)

    def second(j, carry):
        part = product(8 + j)
        stage_one(j).wait_recv()
        send_two[j] = (part + got_one[j].astype(jnp.float32)).astype(send_two.dtype)
        stage_two(j).start()
        return carry

    lax.fori_loop(0, 4, second, 0)

    def third(j, carry):
        own_ref[j] = product(12 + j)
        return carry

    lax.fori_loop(0, 4, third, 0)

    for j in range(4):
        stage_one(4 + j).wait_recv()
        own_ref[j] = own_ref[j] + got_one[4 + j].astype(jnp.float32)
    for j in range(4):
        stage_two(j).wait_recv()
        at = path_sub(j)[1] * width
        out_ref[:, at : at + width] = (own_ref[j] + got_two[j].astype(jnp.float32)).astype(
            out_ref.dtype
        )
    for i in range(8):
        stage_one(i).wait_send()
    for j in range(4):
        stage_two(j).wait_send()


def project(attended, out_weight):
    rows, depth = attended.shape
    features = out_weight.shape[1]
    width = features // 16
    bf16, f32 = jnp.bfloat16, jnp.float32
    return pl.pallas_call(
        project_kernel,
        out_shape=jax.ShapeDtypeStruct((rows, features // 4), bf16),
        in_specs=[pl.BlockSpec(memory_space=pltpu.VMEM), pl.BlockSpec(memory_space=pl.ANY)],
        out_specs=pl.BlockSpec(memory_space=pltpu.VMEM),
        scratch_shapes=[
            pltpu.VMEM((16, depth, width), bf16),
            pltpu.VMEM((8, rows, width), bf16),
            pltpu.VMEM((8, rows, width), bf16),
            pltpu.VMEM((4, rows, width), bf16),
            pltpu.VMEM((4, rows, width), bf16),
            pltpu.VMEM((4, rows, width), f32),
            pltpu.SemaphoreType.DMA((16,)),
            pltpu.SemaphoreType.DMA((8,)),
            pltpu.SemaphoreType.DMA((8,)),
            pltpu.SemaphoreType.DMA((4,)),
            pltpu.SemaphoreType.DMA((4,)),
        ],
        compiler_params=pltpu.CompilerParams(
            collective_id=1, has_side_effects=True, vmem_limit_bytes=60 * 1024 * 1024
        ),
        name="project",
    )(attended, out_weight)


def shards(n_ctx, n_grp, queries, keys, values, out_weight, span_order, document):
    local_heads = queries.shape[1] // HEAD_DIM
    kv_heads = max(1, local_heads // QUERY_GROUP)
    attended = gather_attend(
        queries, keys, values, span_order, document, n_ctx, kv_heads,
        lambda group: group * local_heads // QUERY_GROUP,
    )
    if n_grp == 4:
        return project(attended, out_weight)
    partial_value = jnp.dot(attended, out_weight, preferred_element_type=jnp.float32)
    return lax.psum_scatter(
        partial_value.astype(jnp.bfloat16), "grp", scatter_dimension=1, tiled=True
    )


def solution(mesh):
    in_specs = (P("ctx", "grp"), P("ctx", None), P("ctx", None), P("grp", None), P(), P())
    body = functools.partial(shards, mesh.shape["ctx"], mesh.shape["grp"])
    return jax.shard_map(
        body, mesh=mesh, in_specs=in_specs, out_specs=P("ctx", "grp"), check_vma=False
    )
```

```python
import functools
import math

import jax
import jax.numpy as jnp
from jax import lax
from jax.experimental import pallas as pl
from jax.experimental.pallas import tpu as pltpu
from jax.sharding import PartitionSpec as P

HEAD_DIM = 128
QUERY_GROUP = 8
CORES = 2
MESH = pl.DeviceIdType.MESH
HIDDEN = -1e30
UNROLL = 4
AHEAD = 3


def gather_attend_kernel(
    n_ctx, kv_heads, first_of, order_ref, doc_rows, q_ref, k_hbm, v_hbm, out_ref,
    k_all, v_all, row_doc_ref, bias_ref, max_ref, acc_ref, local_sem, send_sem, recv_sem,
):
    nz = n_ctx // CORES
    me = lax.axis_index("ctx")
    group = lax.axis_index("grp")
    z, core = me // CORES, me % CORES
    partner = z * CORES + 1 - core
    tok_rows, width = k_all.shape[1], k_all.shape[2]
    span = tok_rows // 2
    heads = q_ref.shape[1] // HEAD_DIM
    shared = heads // kv_heads
    start = pl.multiple_of(first_of(group) * HEAD_DIM, HEAD_DIM)
    alls = (k_all, v_all)
    loads = [
        pltpu.make_async_copy(src.at[:, pl.ds(start, width)], dst.at[me], local_sem.at[i])
        for i, (src, dst) in enumerate(((k_hbm, k_all), (v_hbm, v_all)))
    ]
    for load in loads:
        load.start()
    barrier = pltpu.get_barrier_semaphore()
    pl.semaphore_signal(barrier, inc=1, device_id=(partner, group), device_id_type=MESH)

    @pl.when(z > 0)
    def _():
        pl.semaphore_signal(barrier, inc=1, device_id=(me - CORES, group), device_id_type=MESH)

    @pl.when(z < nz - 1)
    def _():
        pl.semaphore_signal(barrier, inc=1, device_id=(me + CORES, group), device_id_type=MESH)

    pl.semaphore_wait(barrier, 1 + jnp.minimum(z, 1) + jnp.minimum(nz - 1 - z, 1))

    def piece(way, part, chip, target):
        block = chip * CORES + core
        return pltpu.make_async_remote_copy(
            src_ref=alls[part].at[block],
            dst_ref=alls[part].at[block],
            send_sem=send_sem.at[way, part, chip],
            recv_sem=recv_sem.at[part, block],
            device_id=(target, group),
            device_id_type=MESH,
        )

    for part in range(2):
        loads[part].wait()

        @pl.when(z < nz - 1)
        def _():
            piece(0, part, z, me + CORES).start()

        @pl.when(z > 0)
        def _():
            piece(1, part, z, me - CORES).start()

        piece(2, part, z, partner).start()

    def arrived(part, chip, from_core):
        block = chip * CORES + from_core
        pltpu.make_async_copy(
            alls[part].at[block], alls[part].at[block], recv_sem.at[part, block]
        ).wait()

    max_ref[...] = jnp.full(max_ref.shape, HIDDEN, jnp.float32)
    acc_ref[...] = jnp.zeros(acc_ref.shape, jnp.float32)
    for r in range(2):
        row_doc_ref[r] = jnp.transpose(
            jnp.broadcast_to(doc_rows[order_ref[me * 2 + r]], (span, span))
        )

    factor = math.log2(math.e) / math.sqrt(HEAD_DIM)
    keys_per_step = CORES * tok_rows
    parts_of_keys = keys_per_step // HEAD_DIM
    row_at = lax.broadcasted_iota(jnp.int32, (span, span), 0)
    col_at = lax.broadcasted_iota(jnp.int32, (span, span), 1)
    near = jnp.minimum(z, nz - 1 - z)
    long_way = jnp.where(z < nz - 1 - z, 1, -1)

    def step(n, carry):
        for part in range(2):

            @pl.when((n > 0) & (z - n >= 0))
            def _():
                arrived(part, z - n, core)

                @pl.when(z < nz - 1)
                def _():
                    piece(0, part, z - n, me + CORES).start()

                piece(2, part, z - n, partner).start()

            @pl.when((n > 0) & (z + n < nz))
            def _():
                arrived(part, z + n, core)

                @pl.when(z > 0)
                def _():
                    piece(1, part, z + n, me - CORES).start()

                piece(2, part, z + n, partner).start()

        away = (n + 1) // 2
        paired = z + away * (1 - 2 * (n % 2))
        chip = jnp.where(n <= 2 * near, paired, z + long_way * (n - near))

        for slot in range(2 * CORES):
            key_span = order_ref[chip * (2 * CORES) + slot]
            key_doc = doc_rows[key_span]
            for r in range(2):
                mine = order_ref[me * 2 + r]
                seen = (key_doc == row_doc_ref[r]) & (
                    key_span * span + col_at <= mine * span + row_at
                )
                bias_ref[r * span : (r + 1) * span, slot * span : (slot + 1) * span] = jnp.where(
                    seen, 0.0, HIDDEN
                )

        for part in range(2):
            arrived(part, chip, 1 - core)

        for h in range(kv_heads):
            cols = slice(h * HEAD_DIM, (h + 1) * HEAD_DIM)

            def some_heads(at, carry):
                key = k_all[pl.ds(chip * CORES, CORES), :, cols].reshape(keys_per_step, HEAD_DIM)
                value = v_all[pl.ds(chip * CORES, CORES), :, cols].reshape(
                    keys_per_step, HEAD_DIM
                )
                value = jnp.concatenate([value, jnp.ones_like(value)], axis=1)
                picked = [h * shared + at * UNROLL + u for u in range(UNROLL)]
                scores = [
                    lax.dot_general(
                        q_ref[:, pl.ds(pl.multiple_of(head * HEAD_DIM, HEAD_DIM), HEAD_DIM)],
                        key,
                        (((1,), (1,)), ((), ())),
                        preferred_element_type=jnp.float32,
                    )
                    + bias_ref[...]
                    for head in picked
                ]
                olds = [max_ref[head] for head in picked]
                sums = [acc_ref[head] for head in picked]
                results = []
                for score, old, total in zip(scores, olds, sums):
                    top = jnp.maximum(old, jnp.max(score, axis=1, keepdims=True))
                    rescale = jnp.exp2((old - top) * factor)
                    probs = jnp.concatenate(
                        [
                            jnp.exp2(
                                (score[:, c * HEAD_DIM : (c + 1) * HEAD_DIM] - top) * factor
                            ).astype(jnp.bfloat16)
                            for c in range(parts_of_keys)
                        ],
                        axis=1,
                    )
                    mixed = jnp.dot(probs, value, preferred_element_type=jnp.float32)
                    both = jnp.concatenate([rescale, rescale], axis=1)
                    results.append((top, total * both + mixed))
                for head, (top, total) in zip(picked, results):
                    max_ref[head] = top
                    acc_ref[head] = total
                return carry

            lax.fori_loop(0, shared // UNROLL, some_heads, 0)
        return carry

    lax.fori_loop(0, nz, step, 0)

    for head in range(heads):
        total = acc_ref[head]
        out_ref[:, head * HEAD_DIM : (head + 1) * HEAD_DIM] = (
            total[:, :HEAD_DIM] / total[:, HEAD_DIM:]
        ).astype(out_ref.dtype)

    for part in range(2):
        for chip in range(nz):
            piece(2, part, chip, partner).wait_send()

            @pl.when((z < nz - 1) & (chip <= z))
            def _():
                piece(0, part, chip, me + CORES).wait_send()

            @pl.when((z > 0) & (chip >= z))
            def _():
                piece(1, part, chip, me - CORES).wait_send()


def gather_attend(queries, keys, values, span_order, document, n_ctx, kv_heads, first_of):
    slots = span_order.shape[0]
    span = document.shape[0] // slots
    rows = queries.shape[0]
    heads = queries.shape[1] // HEAD_DIM
    smem = pl.BlockSpec(memory_space=pltpu.SMEM)
    vmem = pl.BlockSpec(memory_space=pltpu.VMEM)
    hbm = pl.BlockSpec(memory_space=pl.ANY)
    f32, bf16 = jnp.float32, jnp.bfloat16
    return pl.pallas_call(
        functools.partial(gather_attend_kernel, n_ctx, kv_heads, first_of),
        out_shape=jax.ShapeDtypeStruct(queries.shape, queries.dtype),
        in_specs=[smem, vmem, vmem, hbm, hbm],
        out_specs=vmem,
        scratch_shapes=[
            pltpu.VMEM((n_ctx, rows, kv_heads * HEAD_DIM), bf16),
            pltpu.VMEM((n_ctx, rows, kv_heads * HEAD_DIM), bf16),
            pltpu.VMEM((2, span, span), jnp.int32),
            pltpu.VMEM((rows, CORES * rows), f32),
            pltpu.VMEM((heads, rows, HEAD_DIM), f32),
            pltpu.VMEM((heads, rows, 2 * HEAD_DIM), f32),
            pltpu.SemaphoreType.DMA((2,)),
            pltpu.SemaphoreType.DMA((3, 2, n_ctx // CORES)),
            pltpu.SemaphoreType.DMA((2, n_ctx)),
        ],
        compiler_params=pltpu.CompilerParams(collective_id=0, has_side_effects=True),
        name="gather_attend",
    )(span_order, document.reshape(slots, 1, span), queries, keys, values)


def project_kernel(
    att_ref, w_hbm, out_ref, w_buf, send_one, got_one, send_two, got_two, own_ref,
    w_sem, sent_one, recv_one, sent_two, recv_two,
):
    me = lax.axis_index("ctx")
    group = lax.axis_index("grp")
    side = group + 1 - 2 * (group % 2)
    other = (group + 2) % 4
    far = 3 - group
    steps, _, width = w_buf.shape
    block_width = out_ref.shape[1]

    def path_sub(i):
        path = i % 2
        return path, 2 * path + (i // 2) % 2

    def block_of(i):
        path = i % 2
        crossed = jnp.where(path == 1, side, other)
        straight = jnp.where(path == 1, other, side)
        first = jnp.where(i < 4, far, straight)
        return jnp.where(i < 8, first, jnp.where(i < 12, crossed, group))

    def fetch(i, block, sub):
        start = pl.multiple_of(block * block_width + sub * width, width)
        return pltpu.make_async_copy(w_hbm.at[:, pl.ds(start, width)], w_buf.at[i], w_sem.at[i])

    for i in range(AHEAD):
        fetch(i, block_of(i), path_sub(i)[1]).start()

    barrier = pltpu.get_barrier_semaphore()
    for target in (side, other):
        pl.semaphore_signal(barrier, inc=1, device_id=(me, target), device_id_type=MESH)
    pl.semaphore_wait(barrier, 2)

    def product(i):
        fetch(i, group, 0).wait()

        @pl.when(i + AHEAD < steps)
        def _():
            fetch(i + AHEAD, block_of(i + AHEAD), path_sub(i + AHEAD)[1]).start()

        return jnp.dot(att_ref[...], w_buf[i], preferred_element_type=jnp.float32)

    def stage_one(i):
        path = i % 2
        return pltpu.make_async_remote_copy(
            src_ref=send_one.at[i],
            dst_ref=got_one.at[i],
            send_sem=sent_one.at[i],
            recv_sem=recv_one.at[i],
            device_id=(me, (1 - path) * side + path * other),
            device_id_type=MESH,
        )

    def stage_two(j):
        path = j % 2
        return pltpu.make_async_remote_copy(
            src_ref=send_two.at[j],
            dst_ref=got_two.at[j],
            send_sem=sent_two.at[j],
            recv_sem=recv_two.at[j],
            device_id=(me, (1 - path) * other + path * side),
            device_id_type=MESH,
        )

    def first(i, carry):
        send_one[i] = product(i).astype(send_one.dtype)
        stage_one(i).start()
        return carry

    lax.fori_loop(0, 8, first, 0)

    def second(j, carry):
        part = product(8 + j)
        stage_one(j).wait_recv()
        send_two[j] = (part + got_one[j].astype(jnp.float32)).astype(send_two.dtype)
        stage_two(j).start()
        return carry

    lax.fori_loop(0, 4, second, 0)

    def third(j, carry):
        own_ref[j] = product(12 + j)
        return carry

    lax.fori_loop(0, 4, third, 0)

    for j in range(4):
        stage_one(4 + j).wait_recv()
        own_ref[j] = own_ref[j] + got_one[4 + j].astype(jnp.float32)
    for j in range(4):
        stage_two(j).wait_recv()
        at = path_sub(j)[1] * width
        out_ref[:, at : at + width] = (own_ref[j] + got_two[j].astype(jnp.float32)).astype(
            out_ref.dtype
        )
    for i in range(8):
        stage_one(i).wait_send()
    for j in range(4):
        stage_two(j).wait_send()


def project(attended, out_weight):
    rows, depth = attended.shape
    features = out_weight.shape[1]
    width = features // 16
    bf16, f32 = jnp.bfloat16, jnp.float32
    return pl.pallas_call(
        project_kernel,
        out_shape=jax.ShapeDtypeStruct((rows, features // 4), bf16),
        in_specs=[pl.BlockSpec(memory_space=pltpu.VMEM), pl.BlockSpec(memory_space=pl.ANY)],
        out_specs=pl.BlockSpec(memory_space=pltpu.VMEM),
        scratch_shapes=[
            pltpu.VMEM((16, depth, width), bf16),
            pltpu.VMEM((8, rows, width), bf16),
            pltpu.VMEM((8, rows, width), bf16),
            pltpu.VMEM((4, rows, width), bf16),
            pltpu.VMEM((4, rows, width), bf16),
            pltpu.VMEM((4, rows, width), f32),
            pltpu.SemaphoreType.DMA((16,)),
            pltpu.SemaphoreType.DMA((8,)),
            pltpu.SemaphoreType.DMA((8,)),
            pltpu.SemaphoreType.DMA((4,)),
            pltpu.SemaphoreType.DMA((4,)),
        ],
        compiler_params=pltpu.CompilerParams(
            collective_id=1, has_side_effects=True, vmem_limit_bytes=60 * 1024 * 1024
        ),
        name="project",
    )(attended, out_weight)


def shards(n_ctx, n_grp, queries, keys, values, out_weight, span_order, document):
    local_heads = queries.shape[1] // HEAD_DIM
    kv_heads = max(1, local_heads // QUERY_GROUP)
    attended = gather_attend(
        queries, keys, values, span_order, document, n_ctx, kv_heads,
        lambda group: group * local_heads // QUERY_GROUP,
    )
    if n_grp == 4:
        return project(attended, out_weight)
    partial_value = jnp.dot(attended, out_weight, preferred_element_type=jnp.float32)
    return lax.psum_scatter(
        partial_value.astype(jnp.bfloat16), "grp", scatter_dimension=1, tiled=True
    )


def solution(mesh):
    in_specs = (P("ctx", "grp"), P("ctx", None), P("ctx", None), P("grp", None), P(), P())
    body = functools.partial(shards, mesh.shape["ctx"], mesh.shape["grp"])
    return jax.shard_map(
        body, mesh=mesh, in_specs=in_specs, out_specs=P("ctx", "grp"), check_vma=False
    )
```
